8 devices in a mesh: dp: 8 (over z, y, x, core).
Axes of the slice: x: 2, y: 2, z: 1, core: 2. Of those that a mesh axis runs over, the one named last changes fastest.
Arguments:
- img_emb: bfloat16 [16384, 1024], P('dp')
- txt_emb: bfloat16 [16384, 1024], P('dp')
- log_temp: float32 [], replicated
- logit_bias: float32 [], replicated
Outputs:
- output 1: float32 [], replicated
- output 2: float32 [16384, 1024], P('dp')
- output 3: float32 [16384, 1024], P('dp')
- output 4: float32 [], replicated
- output 5: float32 [], replicated
All inputs are finite; a program needn't handle non-finite values.
Results may differ from the reference program's by a relative error of at most 0.001.
Values are sent between devices in bfloat16 or wider.
A program may use at most 1 GiB of HBM per device.

```python
import jax
import jax.numpy as jnp
from jax import lax

EMBED_DIM = 1024
ROWS_DEV = 2048
GROUP_SIZE = 8


def setup_inputs(seed: int = 0) -> dict:
    total_rows = ROWS_DEV * GROUP_SIZE
    num_groups = total_rows // 4
    unit_scale = EMBED_DIM ** -0.5
    rand_keys = jax.random.split(jax.random.key(seed), 10)
    shared_dir = jax.random.normal(rand_keys[0], (EMBED_DIM,), jnp.float32) * unit_scale
    centers = jax.random.normal(rand_keys[1], (num_groups, EMBED_DIM), jnp.float32) * unit_scale
    member = jax.random.randint(rand_keys[2], (total_rows,), 0, num_groups)
    own_part = jax.random.normal(rand_keys[3], (total_rows, EMBED_DIM), jnp.float32) * unit_scale
    img_noise = jax.random.normal(rand_keys[4], (total_rows, EMBED_DIM), jnp.float32) * unit_scale
    txt_noise = jax.random.normal(rand_keys[5], (total_rows, EMBED_DIM), jnp.float32) * unit_scale
    common = 0.47 * centers[member] + 0.28 * own_part
    img_scale = jax.random.uniform(rand_keys[6], (total_rows, 1), jnp.float32, minval=20.0, maxval=60.0)
    txt_scale = jax.random.uniform(rand_keys[7], (total_rows, 1), jnp.float32, minval=20.0, maxval=60.0)
    img_emb = (img_scale * (0.35 * shared_dir + common + 0.76 * img_noise)).astype(jnp.bfloat16)
    txt_emb = (txt_scale * (common - 0.35 * shared_dir + 0.76 * txt_noise)).astype(jnp.bfloat16)
    log_temp = jax.random.uniform(rand_keys[8], (), jnp.float32, minval=4.6, maxval=4.8)
    logit_bias = jax.random.uniform(rand_keys[9], (), jnp.float32, minval=-14.0, maxval=-10.0)
    return {"img_emb": img_emb, "txt_emb": txt_emb, "log_temp": log_temp, "logit_bias": logit_bias}


def normalize_rows(emb):
    emb32 = emb.astype(jnp.float32)
    inv_norm = lax.rsqrt(jnp.sum(emb32 * emb32, axis=-1, keepdims=True))
    return emb32 * inv_norm, inv_norm


def project_back(unit_rows, inv_norm, grad_dir):
    radial = jnp.sum(unit_rows * grad_dir, axis=-1, keepdims=True)
    return (grad_dir - unit_rows * radial) * inv_norm


def reference(img_emb, txt_emb, log_temp, logit_bias):
    total_rows = img_emb.shape[0]
    embed_width = img_emb.shape[1]
    block_rows = min(ROWS_DEV, 512)
    num_blocks = total_rows // block_rows
    img_unit, img_inv = normalize_rows(img_emb)
    txt_unit, txt_inv = normalize_rows(txt_emb)
    img_b = img_unit.astype(jnp.bfloat16)
    txt_b = txt_unit.astype(jnp.bfloat16)
    temp_scale = jnp.exp(log_temp)
    col_ids = jnp.arange(total_rows)

    def row_block(acc_state, block_in):
        x_blk, blk_idx = block_in
        loss_sum, weight_sum, weighted_sim, txt_grad = acc_state
        sim_vals = jnp.dot(x_blk, txt_b.T, preferred_element_type=jnp.float32)
        logits = temp_scale * sim_vals + logit_bias
        row_ids = blk_idx * block_rows + jnp.arange(block_rows)
        label_signs = jnp.where(row_ids[:, None] == col_ids[None, :], 1.0, -1.0)
        weights = -label_signs * jax.nn.sigmoid(-label_signs * logits)
        weights_b = weights.astype(jnp.bfloat16)
        new_state = (
            loss_sum + jnp.sum(jax.nn.softplus(-label_signs * logits)),
            weight_sum + jnp.sum(weights),
            weighted_sim + jnp.sum(weights * sim_vals),
            txt_grad + jnp.dot(weights_b.T, x_blk, preferred_element_type=jnp.float32),
        )
        return new_state, jnp.dot(weights_b, txt_b, preferred_element_type=jnp.float32)

    init_state = (
        jnp.zeros((), jnp.float32),
        jnp.zeros((), jnp.float32),
        jnp.zeros((), jnp.float32),
        jnp.zeros((total_rows, embed_width), jnp.float32),
    )
    blocks_in = (img_b.reshape(num_blocks, block_rows, embed_width), jnp.arange(num_blocks))
    final_state, img_parts = lax.scan(row_block, init_state, blocks_in)
    loss_sum, weight_sum, weighted_sim, txt_grad = final_state
    img_dir = temp_scale * img_parts.reshape(total_rows, embed_width)
    txt_dir = temp_scale * txt_grad
    loss_val = loss_sum / total_rows
    grad_img = project_back(img_unit, img_inv, img_dir)
    grad_txt = project_back(txt_unit, txt_inv, txt_dir)
    grad_log_temp = temp_scale * weighted_sim / total_rows
    grad_bias = weight_sum / total_rows
    return (loss_val, grad_img, grad_txt, grad_log_temp, grad_bias)
```

```python
import functools

import jax
import jax.numpy as jnp
from jax import lax
from jax.experimental import pallas as pl
from jax.experimental.pallas import tpu as pltpu
from jax.sharding import PartitionSpec as P

TILE = 512
STRIP = 64
NT = (((1,), (1,)), ((), ()))
NN = (((1,), (0,)), ((), ()))
TN = (((0,), (0,)), ((), ()))


def dotf(a, b, dims):
    return lax.dot_general(a, b, dims, preferred_element_type=jnp.float32)


def pair_kernel(rows_i, rows_t, has_u, has_v, diag, *refs):
    n_i, n_t = len(rows_i), len(rows_t)
    refs = list(refs)

    def take(n):
        out = refs[:n]
        del refs[:n]
        return out

    (par,) = take(1)
    imgs, txts = take(n_i), take(n_t)
    u_in, v_in = take(has_u), take(has_v)
    (st_in,) = take(1)
    u_out, v_out = take(n_i), take(n_t)
    (st_out,) = take(1)
    img, txt, u_acc, v_acc, s_buf, h_buf, sem_i, sem_t, sem_u, sem_v, sem_uo, sem_vo = refs

    def tiles(arrs, rows):
        out = []
        for arr, n in zip(arrs, rows):
            out += [arr.at[pl.ds(k * TILE, TILE)] for k in range(n // TILE)]
        return out

    img_t, txt_t = tiles(imgs, rows_i), tiles(txts, rows_t)
    mi, mt = len(img_t), len(txt_t)
    at = lambda ref, k: ref.at[pl.ds(k * TILE, TILE)]
    for k in range(max(mi, mt)):
        if k < mi:
            pltpu.make_async_copy(img_t[k], at(img, k), sem_i.at[k]).start()
        if k < mt:
            pltpu.make_async_copy(txt_t[k], at(txt, k), sem_t.at[k]).start()
    v_src, u_src = tiles(v_in, rows_t), tiles(u_in, rows_i)
    nv, nu = len(v_src), len(u_src)
    for k, src in enumerate(v_src):
        pltpu.make_async_copy(src, at(v_acc, k), sem_v.at[k]).start()
    for k, src in enumerate(u_src):
        pltpu.make_async_copy(src, at(u_acc, k), sem_u.at[k]).start()

    def clear(acc, lo, hi):
        def one(k, carry):
            acc[pl.ds(pl.multiple_of(k * 64, 64), 64)] = jnp.zeros((64, acc.shape[1]), jnp.float32)
            return carry

        lax.fori_loop(lo * (TILE // 64), hi * (TILE // 64), one, 0)

    clear(v_acc, nv, mt)
    clear(u_acc, nu, mi)
    st_out[...] = st_in[...]
    ts, bias = par[0], par[1]

    def row(i, carry):
        i0 = pl.multiple_of(i * TILE, TILE)
        a_ref = img.at[pl.ds(i0, TILE)]
        u_ref = u_acc.at[pl.ds(i0, TILE)]
        pltpu.make_async_copy(img_t[0], a_ref, sem_i.at[i]).wait()
        if nu:
            @pl.when(i < nu)
            def _():
                pltpu.make_async_copy(u_ref, u_ref, sem_u.at[i]).wait()

        def col(j, carry):
            j0 = pl.multiple_of(j * TILE, TILE)
            b_ref = txt.at[pl.ds(j0, TILE)]
            v_ref = v_acc.at[pl.ds(j0, TILE)]

            @pl.when(i == 0)
            def _():
                pltpu.make_async_copy(txt_t[0], b_ref, sem_t.at[j]).wait()

            if nv:
                @pl.when(jnp.logical_and(i == 0, j < nv))
                def _():
                    pltpu.make_async_copy(v_ref, v_ref, sem_v.at[j]).wait()

            a, b = a_ref[...], b_ref[...]
            s_buf[...] = dotf(a, b, NT)
            soft = jnp.zeros((8, TILE), jnp.float32)
            wsum = jnp.zeros((8, TILE), jnp.float32)
            wsim = jnp.zeros((8, TILE), jnp.float32)
            for r in range(0, TILE, STRIP):
                s = s_buf[r:r + STRIP]
                logit = s * ts + bias
                if diag:
                    rid = lax.broadcasted_iota(jnp.int32, (STRIP, TILE), 0) + r
                    cid = lax.broadcasted_iota(jnp.int32, (STRIP, TILE), 1)
                    own = jnp.logical_and(rid == cid, i == j)
                    logit = jnp.where(own, -logit, logit)
                e = jnp.exp(jnp.minimum(logit, -logit))
                w = jnp.where(logit >= 0, 1.0, e) / (1.0 + e)
                if diag:
                    w = jnp.where(own, -w, w)
                h_buf[r:r + STRIP] = w.astype(jnp.bfloat16)
                grp = lambda x: [x[k * 8:(k + 1) * 8] for k in range(STRIP // 8)]
                prods = grp(e)
                while len(prods) > 1:
                    prods = [p + q + p * q for p, q in zip(prods[::2], prods[1::2])]
                soft = soft + jnp.log1p(prods[0])
                for x in grp(jnp.maximum(logit, 0.0)):
                    soft = soft + x
                for x in grp(w):
                    wsum = wsum + x
                for x in grp(w * s):
                    wsim = wsim + x
            st_out[0] += soft
            st_out[1] += wsum
            st_out[2] += wsim
            h = h_buf[...]
            u_ref[...] += dotf(h, b, NN)
            v_ref[...] += dotf(h, a, TN)
            return carry

        lax.fori_loop(0, mt, col, 0)
        return carry

    u_dst = tiles(u_out, rows_i)
    if len(u_out) == 1:
        def row_store(i, carry):
            row(i, carry)
            i0 = pl.multiple_of(i * TILE, TILE)
            pltpu.make_async_copy(u_acc.at[pl.ds(i0, TILE)], u_out[0].at[pl.ds(i0, TILE)], sem_uo.at[i]).start()
            return carry

        lax.fori_loop(0, mi, row_store, 0)
    else:
        lax.fori_loop(0, mi, row, 0)
        for k in range(mi):
            pltpu.make_async_copy(at(u_acc, k), u_dst[k], sem_uo.at[k]).start()
    v_dst = tiles(v_out, rows_t)
    for k in range(mt):
        pltpu.make_async_copy(at(v_acc, k), v_dst[k], sem_vo.at[k]).start()
    for k in range(mi):
        pltpu.make_async_copy(at(u_acc, k), u_dst[k], sem_uo.at[k]).wait()
    for k in range(mt):
        pltpu.make_async_copy(at(v_acc, k), v_dst[k], sem_vo.at[k]).wait()


def pair(par, imgs, txts, stats, u_in=(), v_in=(), diag=False):
    width = imgs[0].shape[1]
    rows_i = tuple(x.shape[0] for x in imgs)
    rows_t = tuple(x.shape[0] for x in txts)
    m, n = sum(rows_i), sum(rows_t)
    mi, mt = m // TILE, n // TILE
    any_spec = pl.BlockSpec(memory_space=pl.ANY)
    vmem = pl.BlockSpec(memory_space=pltpu.VMEM)
    ins = [par] + list(imgs) + list(txts)
    specs = [pl.BlockSpec(memory_space=pltpu.SMEM)] + [any_spec] * (len(imgs) + len(txts))
    aliases = {}
    u_in, v_in = list(u_in), list(v_in)
    for k in range(len(u_in)):
        aliases[len(ins) + k] = k
    ins += u_in
    for k in range(len(v_in)):
        aliases[len(ins) + k] = len(imgs) + k
    ins += v_in
    specs += [any_spec] * (len(u_in) + len(v_in))
    ins.append(stats)
    specs.append(vmem)
    f32 = lambda r: jax.ShapeDtypeStruct((r, width), jnp.float32)
    outs = [f32(r) for r in rows_i] + [f32(r) for r in rows_t] + [jax.ShapeDtypeStruct(stats.shape, stats.dtype)]
    dma = lambda k: pltpu.SemaphoreType.DMA((k,))
    call = pl.pallas_call(
        functools.partial(pair_kernel, rows_i, rows_t, len(u_in), len(v_in), diag),
        out_shape=outs,
        in_specs=specs,
        out_specs=[any_spec] * (len(imgs) + len(txts)) + [vmem],
        scratch_shapes=[
            pltpu.VMEM((m, width), jnp.bfloat16),
            pltpu.VMEM((n, width), jnp.bfloat16),
            pltpu.VMEM((m, width), jnp.float32),
            pltpu.VMEM((n, width), jnp.float32),
            pltpu.VMEM((TILE, TILE), jnp.float32),
            pltpu.VMEM((TILE, TILE), jnp.bfloat16),
            dma(mi), dma(mt), dma(mi), dma(mt), dma(mi), dma(mt),
        ],
        input_output_aliases=aliases,
        cost_estimate=pl.CostEstimate(flops=6 * m * n * width, bytes_accessed=6 * (m + n) * width, transcendentals=0),
        compiler_params=pltpu.CompilerParams(vmem_limit_bytes=62 * 1024 * 1024),
    )
    res = call(*ins)
    return res[:len(imgs)], res[len(imgs):-1], res[-1]


def normalize_rows(emb):
    emb32 = emb.astype(jnp.float32)
    inv_norm = lax.rsqrt(jnp.sum(emb32 * emb32, axis=-1, keepdims=True))
    return emb32 * inv_norm, inv_norm


def norm_bf16(emb):
    return normalize_rows(emb)[0].astype(jnp.bfloat16)


def finish_kernel(n_parts, *refs):
    ts_ref, emb_ref = refs[0], refs[1]
    parts, out_ref = refs[2:2 + n_parts], refs[-1]
    emb = emb_ref[...].astype(jnp.float32)
    inv = lax.rsqrt(jnp.sum(emb * emb, axis=-1, keepdims=True))
    unit = emb * inv
    total = parts[0][...]
    for p in parts[1:]:
        total = total + p[...]
    total = total * ts_ref[0]
    radial = jnp.sum(unit * total, axis=-1, keepdims=True)
    out_ref[...] = (total - unit * radial) * inv


def finish(par, emb, parts, chunk, rows, prev):
    width = emb.shape[1]
    step = 256
    per = rows // step
    smem = pl.BlockSpec(memory_space=pltpu.SMEM)
    blk = lambda off: pl.BlockSpec((step, width), lambda i, off=off: (i + off // step, 0))
    ins = [par, emb] + [p for p, _ in parts]
    specs = [smem, blk(chunk * rows)] + [blk(off) for _, off in parts]
    aliases = {}
    if prev is not None:
        aliases = {len(ins): 0}
        ins.append(prev)
        specs.append(pl.BlockSpec(memory_space=pl.ANY))
    return pl.pallas_call(
        functools.partial(finish_kernel, len(parts)),
        out_shape=jax.ShapeDtypeStruct(emb.shape, jnp.float32),
        grid=(per,),
        in_specs=specs,
        out_specs=blk(chunk * rows),
        input_output_aliases=aliases,
        cost_estimate=pl.CostEstimate(flops=40 * rows * width, bytes_accessed=16 * rows * width, transcendentals=0),
        compiler_params=pltpu.CompilerParams(vmem_limit_bytes=32 * 1024 * 1024),
    )(*ins)


def solution(mesh):
    size = mesh.shape['dp']

    def flip(bit):
        return [(k, k ^ bit) for k in range(size)]

    def local_fn(img_emb, txt_emb, log_temp, logit_bias):
        rows = img_emb.shape[0]
        total_rows = rows * size
        nq = 4
        q = rows // nq
        temp_scale = jnp.exp(log_temp)
        par = jnp.stack([temp_scale, logit_bias])
        SIB, XN, YN = 1, 2, 4
        cut = lambda x, k: lax.slice_in_dim(x, k * q, (k + 1) * q)

        def over(x, bit):
            return lax.ppermute(x, 'dp', flip(bit))

        xi = [over(norm_bf16(cut(img_emb, k)), XN) for k in range(nq)]
        yt = [over(norm_bf16(cut(txt_emb, k)), YN) for k in range(nq)]
        own_i, own_t = norm_bf16(img_emb), norm_bf16(txt_emb)
        sib_i = over(own_i, SIB)
        xs = [over(x, SIB) for x in xi]
        st = jnp.zeros((3, 8, TILE), jnp.float32)
        u23, vb, gx, gy = [None] * nq, [None] * nq, [None] * nq, [None] * nq

        def send_u(k):
            mine, other = u23[k]
            gx[k] = over(mine + over(other, SIB), XN)

        def send_v(k):
            gy[k] = over(vb[k], YN)

        (u0,), (va,), st = pair(par, [own_i], [own_t], st, diag=True)
        (u0, u1), (vb[0],), st = pair(par, [own_i, sib_i], [yt[0]], st, u_in=[u0])
        u23[0], (va,), st = pair(par, [xi[0], xs[0]], [own_t], st, v_in=[va])
        (u0, u1), (vb[1],), st = pair(par, [own_i, sib_i], [yt[1]], st, u_in=[u0, u1])
        u23[1], (va,), st = pair(par, [xi[1], xs[1]], [own_t], st, v_in=[va])
        u23[0], vb, st = pair(par, [xi[0], xs[0]], yt, st, u_in=u23[0], v_in=vb[:2])
        vb = list(vb)
        send_u(0)
        imgs = [xi[1], xs[1], xi[2], xs[2], xi[3], xs[3]]
        res, (vb[0],), st = pair(par, imgs, [yt[0]], st, u_in=u23[1], v_in=[vb[0]])
        u23[1], u23[2], u23[3] = res[0:2], res[2:4], res[4:6]
        send_v(0)
        u23[1], vb[1:], st = pair(par, [xi[1], xs[1]], yt[1:], st, u_in=u23[1], v_in=vb[1:])
        send_u(1)
        res, (vb[1],), st = pair(par, [xi[2], xs[2], xi[3], xs[3]], [yt[1]], st,
                                 u_in=list(u23[2]) + list(u23[3]), v_in=[vb[1]])
        u23[2], u23[3] = res[0:2], res[2:4]
        send_v(1)
        for k in (2, 3):
            u23[k], (va,), st = pair(par, [xi[k], xs[k]], [own_t], st, u_in=u23[k], v_in=[va])
            u23[k], vb[2:], st = pair(par, [xi[k], xs[k]], yt[2:], st, u_in=u23[k], v_in=vb[2:])
            send_u(k)
        for k in (2, 3):
            (u0, u1), (vb[k],), st = pair(par, [own_i, sib_i], [yt[k]], st, u_in=[u0, u1], v_in=[vb[k]])
            send_v(k)
        (u1,), (va,), st = pair(par, [sib_i], [own_t], st, u_in=[u1], v_in=[va])
        us = over(u1, SIB)
        sums = lax.psum(jnp.sum(st, axis=(1, 2)), 'dp') / total_rows
        grad_img = grad_txt = None
        for k in range(nq):
            grad_img = finish(par, img_emb, [(u0, k * q), (us, k * q), (gx[k], 0)], k, q, grad_img)
            grad_txt = finish(par, txt_emb, [(va, k * q), (gy[k], 0)], k, q, grad_txt)
        return sums[0], grad_img, grad_txt, temp_scale * sums[2], sums[1]

    return jax.shard_map(
        local_fn,
        mesh=mesh,
        in_specs=(P('dp', None), P('dp', None), P(), P()),
        out_specs=(P(), P('dp', None), P('dp', None), P(), P()),
        check_vma=False,
    )
```

```python
import functools

import jax
import jax.numpy as jnp
from jax import lax
from jax.experimental import pallas as pl
from jax.experimental.pallas import tpu as pltpu
from jax.sharding import PartitionSpec as P

TILE = 512
STRIP = 64
NQ = 4
NT = (((1,), (1,)), ((), ()))
NN = (((1,), (0,)), ((), ()))
TN = (((0,), (0,)), ((), ()))
SIB, XN, YN = 1, 2, 4

SEGMENTS = (
    (0, 1, 0, 4, 16),
    (0, 1, 4, 1, 8),
    (8, 4, 0, 4, 8),
    (8, 4, 4, 2, 4),
    (9, 4, 4, 2, 4),
    (10, 4, 4, 1, 2),
    (8, 4, 6, 1, 2),
    (8, 4, 7, 1, 2),
    (11, 4, 4, 1, 2),
    (9, 4, 6, 2, 4),
    (9, 4, 0, 4, 8),
    (0, 1, 5, 1, 8),
    (10, 4, 5, 1, 2),
    (11, 4, 5, 1, 2),
    (10, 4, 6, 2, 4),
    (10, 4, 0, 4, 8),
    (0, 1, 6, 1, 8),
    (11, 4, 6, 1, 2),
    (11, 4, 0, 4, 8),
    (11, 4, 7, 1, 2),
    (0, 1, 7, 1, 8),
    (4, 1, 0, 4, 16),
)
FORWARD_AT = (13, 23, 34, 43)


def order():
    seq = []
    for i0, istep, j0, nj, n in SEGMENTS:
        seq += [(i0 + istep * (t // nj), j0 + t % nj) for t in range(n)]
    return seq


SEQ = order()
STEPS = len(SEQ)
assert STEPS == 128 and len(set(SEQ)) == 128


def tile_of(step):
    start = 0
    vals = None
    for i0, istep, j0, nj, n in SEGMENTS:
        cur = (i0, istep, j0, nj, start)
        if vals is None:
            vals = [jnp.int32(c) for c in cur]
        else:
            vals = [jnp.where(step >= start, c, v) for c, v in zip(cur, vals)]
        start += n
    i0, istep, j0, nj, st = vals
    t = step - st
    q = jnp.where(nj == 1, t, jnp.where(nj == 2, t // 2, t // 4))
    return i0 + istep * q, j0 + (t - q * nj)


def dotf(a, b, dims):
    return lax.dot_general(a, b, dims, preferred_element_type=jnp.float32)


def at(ref, k):
    start = k * TILE
    if not isinstance(start, int):
        start = pl.multiple_of(start, TILE)
    return ref.at[pl.ds(start, TILE)]


def main_kernel(par, img_in, txt_in, img_all, txt_all, u_own, v_own, u_sib, u_far, v_far, u_tmp, st_out,
                img_s, txt_s, u_acc, v_acc, tmp, s_buf, h_buf, st_rx,
                ld_i, ld_t, io, s_sem, r_sem, st_sem):
    me = lax.axis_index('dp')
    bit = lambda b: jnp.where((me // b) % 2 == 0, me + b, me - b)
    peer = {b: bit(b) for b in (SIB, XN, YN)}

    GX, GY, GS, FX, SU, SX, SV, US = (NQ * k for k in range(8))

    def remote(src, dst, cid, b):
        return pltpu.make_async_remote_copy(
            src_ref=src, dst_ref=dst, send_sem=s_sem.at[cid], recv_sem=r_sem.at[cid],
            device_id=(peer[b],), device_id_type=pl.DeviceIdType.MESH)

    def copy_of(kind, k):
        if kind == GX:
            return remote(at(img_all, k), at(img_all, 8 + k), GX + k, XN)
        if kind == GY:
            return remote(at(txt_all, k), at(txt_all, 4 + k), GY + k, YN)
        if kind == GS:
            return remote(at(img_all, k), at(img_all, 4 + k), GS + k, SIB)
        if kind == FX:
            return remote(at(img_all, 8 + k), at(img_all, 12 + k), FX + k, SIB)
        if kind == SU:
            return remote(at(u_acc, 12 + k), at(u_tmp, k), SU + k, SIB)
        if kind == SX:
            return remote(at(u_acc, 8 + k), at(u_far, k), SX + k, XN)
        if kind == SV:
            return remote(at(v_acc, 4 + k), at(v_far, k), SV + k, YN)
        return remote(at(u_acc, 4 + k), at(u_sib, k), US + k, SIB)

    def load_raw(t):
        return (pltpu.make_async_copy(at(img_in, t), img_s.at[t % 2], ld_i.at[t % 2]),
                pltpu.make_async_copy(at(txt_in, t), txt_s.at[t % 2], ld_t.at[t % 2]))

    def store_unit(t):
        return (pltpu.make_async_copy(img_s.at[t % 2], at(img_all, t), io.at[2 * (t % 2)]),
                pltpu.make_async_copy(txt_s.at[t % 2], at(txt_all, t), io.at[2 * (t % 2) + 1]))

    def unit_rows(buf):
        def one(k, carry):
            sl = pl.ds(pl.multiple_of(k * STRIP, STRIP), STRIP)
            x = buf[sl, :].astype(jnp.float32)
            inv = lax.rsqrt(jnp.sum(x * x, axis=-1, keepdims=True))
            buf[sl, :] = (x * inv).astype(jnp.bfloat16)
            return carry
        lax.fori_loop(0, TILE // STRIP, one, 0)

    for t in (0, 1):
        for c in load_raw(t):
            c.start()
    barrier = pltpu.get_barrier_semaphore()
    for b in (SIB, XN, YN):
        pl.semaphore_signal(barrier, inc=1, device_id=(peer[b],), device_id_type=pl.DeviceIdType.MESH)
    pl.semaphore_wait(barrier, 3)

    def send_unit(t):
        for c in store_unit(t):
            c.wait()
        for kind in (GX, GY, GS):
            copy_of(kind, t).start()

    for t in range(NQ):
        for c in load_raw(t):
            c.wait()
        unit_rows(img_s.at[t % 2])
        unit_rows(txt_s.at[t % 2])
        for c in store_unit(t):
            c.start()
        if t == 0:
            send_unit(0)
        if t >= 2:
            send_unit(t - 1)
        if 1 <= t + 1 < NQ and t >= 1:
            for c in load_raw(t + 1):
                c.start()
    send_unit(NQ - 1)

    def clear(acc, n):
        def one(k, carry):
            acc[pl.ds(pl.multiple_of(k * 64, 64), 64)] = jnp.zeros((64, acc.shape[1]), jnp.float32)
            return carry
        lax.fori_loop(0, n * (TILE // 64), one, 0)

    ts, bias = par[0], par[1]

    def fetch(i, j, slot):
        return (pltpu.make_async_copy(at(img_all, i), img_s.at[slot], ld_i.at[slot]),
                pltpu.make_async_copy(at(txt_all, j), txt_s.at[slot], ld_t.at[slot]))

    for c in fetch(SEQ[0][0], SEQ[0][1], 0):
        c.start()
    clear(u_acc, 16)
    clear(v_acc, 8)
    st_out[...] = jnp.zeros_like(st_out)

    events = {}
    add = lambda s, f: events.setdefault(s, []).append(f)
    first_i, first_j, last_i, last_j = {}, {}, {}, {}
    for s, (i, j) in enumerate(SEQ):
        first_i.setdefault(i, s)
        first_j.setdefault(j, s)
        last_i[i], last_j[j] = s, s
    wait_in = lambda kind, k: (lambda: copy_of(kind, k).wait_recv())
    start = lambda kind, k: (lambda: copy_of(kind, k).start())
    tmp_load = lambda k: pltpu.make_async_copy(at(u_tmp, k), tmp, io.at[0])

    def reduce_begin(k):
        copy_of(SU, k).wait_recv()
        tmp_load(k).start()

    def reduce_end(k):
        tmp_load(k).wait()

        def one(n, carry):
            sl = pl.ds(pl.multiple_of(n * 64, 64), 64)
            dst = pl.ds(pl.multiple_of((8 + k) * TILE + n * 64, 64), 64)
            u_acc[dst, :] = u_acc[dst, :] + tmp[sl, :]
            return carry
        lax.fori_loop(0, TILE // 64, one, 0)
        copy_of(SX, k).start()

    for k in range(NQ):
        add(FORWARD_AT[k], wait_in(GX, k))
        add(FORWARD_AT[k], start(FX, k))
        add(first_i[4 + k] - 1, wait_in(GS, k))
        add(first_i[12 + k] - 1, wait_in(FX, k))
        add(first_j[4 + k] - 1, wait_in(GY, k))
        assert FORWARD_AT[k] < first_i[8 + k]
        done = max(last_i[8 + k], last_i[12 + k]) + 1
        add(done, start(SU, k))
        add(done + 2, functools.partial(reduce_begin, k))
        add(done + 3, functools.partial(reduce_end, k))
        add(last_j[4 + k] + 1, start(SV, k))
        add(last_i[4 + k] + 1, start(US, k))
        add(last_i[k] + 1, lambda k=k: pltpu.make_async_copy(at(u_acc, k), at(u_own, k), io.at[4 + k]).start())
    late = [f for s in sorted(events) if s >= STEPS for f in events[s]]
    events = {s: fs for s, fs in sorted(events.items()) if s < STEPS}

    def body(step, carry):
        i, j, slot = carry
        any_event = functools.reduce(jnp.logical_or, [step == s for s in events])

        @pl.when(any_event)
        def _():
            for s, fs in events.items():
                @pl.when(step == s)
                def _(fs=fs):
                    for f in fs:
                        f()

        ni, nj = tile_of(step + 1)
        nslot = 1 - slot

        @pl.when(step + 1 < STEPS)
        def _():
            for c in fetch(ni, nj, nslot):
                c.start()
        for c in fetch(i, j, slot):
            c.wait()

        a_ref, b_ref = img_s.at[slot], txt_s.at[slot]
        u_ref, v_ref = at(u_acc, i), at(v_acc, j)
        a, b = a_ref[...], b_ref[...]
        s_buf[...] = dotf(a, b, NT)
        soft = jnp.zeros((8, TILE), jnp.float32)
        wsum = jnp.zeros((8, TILE), jnp.float32)
        wsim = jnp.zeros((8, TILE), jnp.float32)
        own_tile = jnp.logical_and(i == j, i < 4)
        grp = lambda x: [x[k * 8:(k + 1) * 8] for k in range(STRIP // 8)]
        for r in range(0, TILE, STRIP):
            c0 = (r // 128) * 128
            rid = lax.broadcasted_iota(jnp.int32, (STRIP, 128), 0) + (r - c0)
            own = jnp.logical_and(rid == lax.broadcasted_iota(jnp.int32, (STRIP, 128), 1), own_tile)

            def flip(x):
                mid = x[:, c0:c0 + 128]
                parts = [x[:, :c0]] * (c0 > 0) + [jnp.where(own, -mid, mid)] + [x[:, c0 + 128:]] * (c0 + 128 < TILE)
                return jnp.concatenate(parts, axis=1)

            s = s_buf[r:r + STRIP]
            logit = flip(s * ts + bias)
            e = jnp.exp(jnp.minimum(logit, -logit))
            w = flip(jnp.where(logit >= 0, 1.0, e) / (1.0 + e))
            h_buf[r:r + STRIP] = w.astype(jnp.bfloat16)
            prods = grp(e)
            while len(prods) > 1:
                prods = [p + q + p * q for p, q in zip(prods[::2], prods[1::2])]
            soft = soft + jnp.log1p(prods[0])
            for x in grp(jnp.maximum(logit, 0.0)):
                soft = soft + x
            for x in grp(w):
                wsum = wsum + x
            for x in grp(w * s):
                wsim = wsim + x
        st_out[0] += soft
        st_out[1] += wsum
        st_out[2] += wsim
        h = h_buf[...]
        u_ref[...] += dotf(h, b, NN)
        v_ref[...] += dotf(h, a, TN)
        return ni, nj, nslot

    lax.fori_loop(0, STEPS, body, (jnp.int32(SEQ[0][0]), jnp.int32(SEQ[0][1]), jnp.int32(0)))
    for f in late:
        f()
    v_store = [pltpu.make_async_copy(at(v_acc, k), at(v_own, k), io.at[8 + k]) for k in range(NQ)]
    for c in v_store:
        c.start()
    for n, b in enumerate((SIB, XN, YN)):
        c = pltpu.make_async_remote_copy(
            src_ref=st_out, dst_ref=st_rx.at[n], send_sem=st_sem.at[n], recv_sem=st_sem.at[3 + n],
            device_id=(peer[b],), device_id_type=pl.DeviceIdType.MESH)
        c.start()
        c.wait()
        st_out[...] = st_out[...] + st_rx[n]
    for c in v_store:
        c.wait()
    for k in range(NQ):
        pltpu.make_async_copy(at(u_acc, k), at(u_own, k), io.at[4 + k]).wait()
        for kind in (GX, GY, GS, FX, SU, SX, SV, US):
            copy_of(kind, k).wait_send()
        for kind in (US, SX, SV):
            copy_of(kind, k).wait_recv()


def main_call(par, img_emb, txt_emb):
    rows, width = img_emb.shape
    any_spec = pl.BlockSpec(memory_space=pl.ANY)
    f32 = jax.ShapeDtypeStruct((rows, width), jnp.float32)
    dma = lambda k: pltpu.SemaphoreType.DMA((k,))
    outs = [
        jax.ShapeDtypeStruct((4 * rows, width), jnp.bfloat16),
        jax.ShapeDtypeStruct((2 * rows, width), jnp.bfloat16),
        f32, f32, f32, f32, f32, f32,
        jax.ShapeDtypeStruct((3, 8, TILE), jnp.float32),
    ]
    return pl.pallas_call(
        main_kernel,
        out_shape=outs,
        in_specs=[pl.BlockSpec(memory_space=pltpu.SMEM), any_spec, any_spec],
        out_specs=[any_spec] * 8 + [pl.BlockSpec(memory_space=pltpu.VMEM)],
        scratch_shapes=[
            pltpu.VMEM((2, TILE, width), jnp.bfloat16),
            pltpu.VMEM((2, TILE, width), jnp.bfloat16),
            pltpu.VMEM((16 * TILE, width), jnp.float32),
            pltpu.VMEM((8 * TILE, width), jnp.float32),
            pltpu.VMEM((TILE, width), jnp.float32),
            pltpu.VMEM((TILE, TILE), jnp.float32),
            pltpu.VMEM((TILE, TILE), jnp.bfloat16),
            pltpu.VMEM((3, 3, 8, TILE), jnp.float32),
            dma(2), dma(2), dma(12), dma(32), dma(32), dma(6),
        ],
        cost_estimate=pl.CostEstimate(flops=6 * 8 * rows * rows * width, bytes_accessed=1 << 28, transcendentals=0),
        compiler_params=pltpu.CompilerParams(
            collective_id=0, has_side_effects=True, vmem_limit_bytes=67043328),
        name="pairs",
    )(par, img_emb, txt_emb)


def finish_kernel(n_parts, *refs):
    ts_ref, emb_ref = refs[0], refs[1]
    parts, out_ref = refs[2:2 + n_parts], refs[-1]
    emb = emb_ref[...].astype(jnp.float32)
    inv = lax.rsqrt(jnp.sum(emb * emb, axis=-1, keepdims=True))
    unit = emb * inv
    total = parts[0][...]
    for p in parts[1:]:
        total = total + p[...]
    total = total * ts_ref[0]
    radial = jnp.sum(unit * total, axis=-1, keepdims=True)
    out_ref[...] = (total - unit * radial) * inv


def finish(par, emb, parts, name):
    rows, width = emb.shape
    step = 256
    blk = pl.BlockSpec((step, width), lambda i: (i, 0))
    return pl.pallas_call(
        functools.partial(finish_kernel, len(parts)),
        out_shape=jax.ShapeDtypeStruct(emb.shape, jnp.float32),
        grid=(rows // step,),
        in_specs=[pl.BlockSpec(memory_space=pltpu.SMEM)] + [blk] * (1 + len(parts)),
        out_specs=blk,
        cost_estimate=pl.CostEstimate(flops=40 * rows * width, bytes_accessed=16 * rows * width, transcendentals=0),
        compiler_params=pltpu.CompilerParams(vmem_limit_bytes=32 * 1024 * 1024),
        name=name,
    )(par, emb, *parts)


def solution(mesh):
    size = mesh.shape['dp']

    def local_fn(img_emb, txt_emb, log_temp, logit_bias):
        total_rows = img_emb.shape[0] * size
        temp_scale = jnp.exp(log_temp)
        par = jnp.stack([temp_scale, logit_bias])
        _, _, u_own, v_own, u_sib, u_far, v_far, _, st = main_call(par, img_emb, txt_emb)
        sums = jnp.sum(st, axis=(1, 2)) / total_rows
        grad_img = finish(par, img_emb, [u_own, u_sib, u_far], "fin_i")
        grad_txt = finish(par, txt_emb, [v_own, v_far], "fin_t")
        return sums[0], grad_img, grad_txt, temp_scale * sums[2], sums[1]

    return jax.shard_map(
        local_fn,
        mesh=mesh,
        in_specs=(P('dp', None), P('dp', None), P(), P()),
        out_specs=(P(), P('dp', None), P('dp', None), P(), P()),
        check_vma=False,
    )
```

```python
import functools

import jax
import jax.numpy as jnp
from jax import lax
from jax.experimental import pallas as pl
from jax.experimental.pallas import tpu as pltpu
from jax.sharding import PartitionSpec as P

TILE = 512
STRIP = 64
NQ = 4
NT = (((1,), (1,)), ((), ()))
NN = (((1,), (0,)), ((), ()))
TN = (((0,), (0,)), ((), ()))
SIB, XN, YN = 1, 2, 4

SEGMENTS = (
    (0, 1, 0, 4, 4),
    (0, 1, 4, 1, 4),
    (4, 1, 0, 4, 4),
    (4, 1, 4, 2, 4),
    (4, 1, 6, 1, 1),
    (5, 1, 0, 4, 4),
    (6, 1, 4, 1, 1),
    (4, 1, 7, 1, 1),
    (7, 1, 4, 1, 1),
    (5, 1, 6, 2, 2),
    (0, 1, 5, 1, 4),
    (6, 1, 5, 1, 2),
    (6, 1, 0, 4, 4),
    (6, 1, 6, 2, 2),
    (0, 1, 6, 1, 4),
    (7, 1, 6, 1, 1),
    (7, 1, 0, 4, 4),
    (7, 1, 7, 1, 1),
    (0, 1, 7, 1, 4),
    (1, 1, 0, 4, 12),
)
FORWARD_AT = (4, 10, 18, 21)


def order():
    seq = []
    for i0, istep, j0, nj, n in SEGMENTS:
        seq += [(i0 + istep * (t // nj), j0 + t % nj) for t in range(n)]
    return seq


SEQ = order()
STEPS = len(SEQ)
assert STEPS == 64 and len(set(SEQ)) == 64


def tile_of(step):
    start = 0
    vals = None
    for i0, istep, j0, nj, n in SEGMENTS:
        cur = (i0, istep, j0, nj, start)
        if vals is None:
            vals = [jnp.int32(c) for c in cur]
        else:
            vals = [jnp.where(step >= start, c, v) for c, v in zip(cur, vals)]
        start += n
    i0, istep, j0, nj, st = vals
    t = step - st
    q = jnp.where(nj == 1, t, jnp.where(nj == 2, t // 2, t // 4))
    return i0 + istep * q, j0 + (t - q * nj)


def dotf(a, b, dims):
    return lax.dot_general(a, b, dims, preferred_element_type=jnp.float32)


def at(ref, k, n=TILE):
    start = k * n
    if not isinstance(start, int):
        start = pl.multiple_of(start, n)
    return ref.at[pl.ds(start, n)]


def main_kernel(par, img_in, txt_in, g_img, g_txt, img_all, txt_all, u_sib, u_far, v_far, u_tmp, st_out,
                img_s, txt_s, u_acc, v_acc, tmp, s_buf, h_buf, st_rx,
                ld_i, ld_t, io, s_sem, r_sem, st_sem):
    me = lax.axis_index('dp')
    bit = lambda b: jnp.where((me // b) % 2 == 0, me + b, me - b)
    peer = {b: bit(b) for b in (SIB, XN, YN)}

    GX, GY, GS, FX, SU, SX, SV, US = (NQ * k for k in range(8))

    def remote(src, dst, cid, b):
        return pltpu.make_async_remote_copy(
            src_ref=src, dst_ref=dst, send_sem=s_sem.at[cid], recv_sem=r_sem.at[cid],
            device_id=(peer[b],), device_id_type=pl.DeviceIdType.MESH)

    def copy_of(kind, k):
        if kind == GX:
            return remote(at(img_all, 2 * k), at(img_all, 8 + 2 * k), GX + k, XN)
        if kind == GY:
            return remote(at(txt_all, k), at(txt_all, 4 + k), GY + k, YN)
        if kind == GS:
            return remote(at(img_all, 2 * k), at(img_all, 2 * k + 1), GS + k, SIB)
        if kind == FX:
            return remote(at(img_all, 8 + 2 * k), at(img_all, 9 + 2 * k), FX + k, SIB)
        if kind == SU:
            return remote(at(u_acc, 9 + 2 * k), at(u_tmp, k), SU + k, SIB)
        if kind == SX:
            return remote(at(u_acc, 8 + 2 * k), at(u_far, k), SX + k, XN)
        if kind == SV:
            return remote(at(v_acc, 4 + k), at(v_far, k), SV + k, YN)
        return remote(at(u_acc, 2 * k + 1), at(u_sib, k), US + k, SIB)

    raw_i = lambda t: img_s.at[t % 2, pl.ds(0, TILE)]

    def load_raw(t):
        return (pltpu.make_async_copy(at(img_in, t), raw_i(t), ld_i.at[t % 2]),
                pltpu.make_async_copy(at(txt_in, t), txt_s.at[t % 2], ld_t.at[t % 2]))

    def store_unit(t):
        return (pltpu.make_async_copy(raw_i(t), at(img_all, 2 * t), io.at[2 * (t % 2)]),
                pltpu.make_async_copy(txt_s.at[t % 2], at(txt_all, t), io.at[2 * (t % 2) + 1]))

    def unit_rows(buf):
        def one(k, carry):
            sl = pl.ds(pl.multiple_of(k * STRIP, STRIP), STRIP)
            x = buf[sl, :].astype(jnp.float32)
            inv = lax.rsqrt(jnp.sum(x * x, axis=-1, keepdims=True))
            buf[sl, :] = (x * inv).astype(jnp.bfloat16)
            return carry
        lax.fori_loop(0, TILE // STRIP, one, 0)

    for t in (0, 1):
        for c in load_raw(t):
            c.start()
    barrier = pltpu.get_barrier_semaphore()
    for b in (SIB, XN, YN):
        pl.semaphore_signal(barrier, inc=1, device_id=(peer[b],), device_id_type=pl.DeviceIdType.MESH)
    pl.semaphore_wait(barrier, 3)

    def send_unit(t):
        for c in store_unit(t):
            c.wait()
        for kind in (GX, GY, GS):
            copy_of(kind, t).start()

    for t in range(NQ):
        for c in load_raw(t):
            c.wait()
        unit_rows(raw_i(t))
        unit_rows(txt_s.at[t % 2])
        for c in store_unit(t):
            c.start()
        if t == 0:
            send_unit(0)
        if t >= 2:
            send_unit(t - 1)
        if 1 <= t + 1 < NQ and t >= 1:
            for c in load_raw(t + 1):
                c.start()
    send_unit(NQ - 1)

    def clear(acc, n):
        def one(k, carry):
            acc[pl.ds(pl.multiple_of(k * 64, 64), 64)] = jnp.zeros((64, acc.shape[1]), jnp.float32)
            return carry
        lax.fori_loop(0, n * (TILE // 64), one, 0)

    ts, bias = par[0], par[1]

    def fetch(i, j, slot):
        return (pltpu.make_async_copy(at(img_all, i, 2 * TILE), img_s.at[slot], ld_i.at[slot]),
                pltpu.make_async_copy(at(txt_all, j), txt_s.at[slot], ld_t.at[slot]))

    clear(u_acc, 16)
    clear(v_acc, 8)
    copy_of(GS, 0).wait_recv()
    for c in fetch(SEQ[0][0], SEQ[0][1], 0):
        c.start()
    st_out[...] = jnp.zeros_like(st_out)

    events = {}
    add = lambda s, f: events.setdefault(s, []).append(f)
    first_i, first_j, last_i, last_j = {}, {}, {}, {}
    for s, (i, j) in enumerate(SEQ):
        first_i.setdefault(i, s)
        first_j.setdefault(j, s)
        last_i[i], last_j[j] = s, s
    wait_in = lambda kind, k: (lambda: copy_of(kind, k).wait_recv())
    start = lambda kind, k: (lambda: copy_of(kind, k).start())
    tmp_load = lambda k: pltpu.make_async_copy(at(u_tmp, k), tmp, io.at[0])

    def reduce_end(k):
        tmp_load(k).wait()

        def one(n, carry):
            sl = pl.ds(pl.multiple_of(n * 64, 64), 64)
            dst = pl.ds(pl.multiple_of((8 + 2 * k) * TILE + n * 64, 64), 64)
            u_acc[dst, :] = u_acc[dst, :] + tmp[sl, :]
            return carry
        lax.fori_loop(0, TILE // 64, one, 0)
        copy_of(SX, k).start()

    def reduce_far(k):
        copy_of(SU, k).wait_recv()
        tmp_load(k).start()
        reduce_end(k)

    for k in range(NQ):
        add(FORWARD_AT[k], wait_in(GX, k))
        add(FORWARD_AT[k], start(FX, k))
        if k:
            add(first_i[k] - 1, wait_in(GS, k))
        add(first_i[4 + k] - 1, wait_in(FX, k))
        add(first_j[4 + k] - 1, wait_in(GY, k))
        assert FORWARD_AT[k] < first_i[4 + k]
        add(last_i[4 + k] + 1, start(SU, k))
        add(last_i[4 + k] + 2, functools.partial(reduce_far, k))
        add(last_j[4 + k] + 1, start(SV, k))
        add(last_i[k] + 1, start(US, k))
    late = [f for s in sorted(events) if s >= STEPS for f in events[s]]
    events = {s: fs for s, fs in sorted(events.items()) if s < STEPS}

    def body(step, carry):
        i, j, slot = carry
        any_event = functools.reduce(jnp.logical_or, [step == s for s in events])

        @pl.when(any_event)
        def _():
            for s, fs in events.items():
                @pl.when(step == s)
                def _(fs=fs):
                    for f in fs:
                        f()

        ni, nj = tile_of(step + 1)
        nslot = 1 - slot

        @pl.when(step + 1 < STEPS)
        def _():
            for c in fetch(ni, nj, nslot):
                c.start()
        for c in fetch(i, j, slot):
            c.wait()

        a_ref, b_ref = img_s.at[slot], txt_s.at[slot]
        u_ref, v_ref = at(u_acc, i, 2 * TILE), at(v_acc, j)
        s_buf[...] = dotf(a_ref[...], b_ref[...], NT)
        soft = jnp.zeros((8, TILE), jnp.float32)
        wsum = jnp.zeros((8, TILE), jnp.float32)
        wsim = jnp.zeros((8, TILE), jnp.float32)
        own_tile = jnp.logical_and(i == j, i < 4)
        grp = lambda x: [x[k * 8:(k + 1) * 8] for k in range(STRIP // 8)]
        for r in range(0, 2 * TILE, STRIP):
            c0 = (r // 128) * 128
            rid = lax.broadcasted_iota(jnp.int32, (STRIP, 128), 0) + (r - c0)
            own = jnp.logical_and(rid == lax.broadcasted_iota(jnp.int32, (STRIP, 128), 1), own_tile)

            def flip(x):
                if r >= TILE:
                    return x
                mid = x[:, c0:c0 + 128]
                parts = [x[:, :c0]] * (c0 > 0) + [jnp.where(own, -mid, mid)] + [x[:, c0 + 128:]] * (c0 + 128 < TILE)
                return jnp.concatenate(parts, axis=1)

            s = s_buf[r:r + STRIP]
            logit = flip(s * ts + bias)
            e = jnp.exp(jnp.minimum(logit, -logit))
            w = flip(jnp.where(logit >= 0, 1.0, e) / (1.0 + e))
            h_buf[r:r + STRIP] = w.astype(jnp.bfloat16)
            prods = grp(e)
            while len(prods) > 1:
                prods = [p + q + p * q for p, q in zip(prods[::2], prods[1::2])]
            soft = soft + jnp.log1p(prods[0])
            for x in grp(jnp.maximum(logit, 0.0)):
                soft = soft + x
            for x in grp(w):
                wsum = wsum + x
            for x in grp(w * s):
                wsim = wsim + x
        st_out[0] += soft
        st_out[1] += wsum
        st_out[2] += wsim
        h = h_buf[...]
        u_ref[...] += dotf(h, b_ref[...], NN)
        v_ref[...] += dotf(h, a_ref[...], TN)
        return ni, nj, nslot

    lax.fori_loop(0, STEPS, body, (jnp.int32(SEQ[0][0]), jnp.int32(SEQ[0][1]), jnp.int32(0)))
    for f in late:
        f()
    for n, b in enumerate((SIB, XN, YN)):
        c = pltpu.make_async_remote_copy(
            src_ref=st_out, dst_ref=st_rx.at[n], send_sem=st_sem.at[n], recv_sem=st_sem.at[3 + n],
            device_id=(peer[b],), device_id_type=pl.DeviceIdType.MESH)
        c.start()
        c.wait()
        st_out[...] = st_out[...] + st_rx[n]

    def loads(n, item):
        txt, k = item
        emb = pltpu.make_async_copy(at(txt_in if txt else img_in, k), raw_i(n), ld_i.at[n % 2])
        if txt:
            return emb, pltpu.make_async_copy(at(v_far, k), at(v_acc, 4 + k), io.at[4 + n % 2])
        return (emb, pltpu.make_async_copy(at(u_far, k), at(u_acc, 8 + 2 * k), io.at[4 + n % 2]),
                pltpu.make_async_copy(at(u_sib, k), at(u_acc, 9 + 2 * k), io.at[6 + n % 2]))

    def load_item(n, item):
        txt, k = item
        for kind in ((SV,) if txt else (US, SX)):
            copy_of(kind, k).wait_recv()
        for kind in ((SV,) if txt else (SU, SX)):
            copy_of(kind, k).wait_send()
        for c in loads(n, item):
            c.start()

    def store_item(item):
        txt, k = item
        if txt:
            return pltpu.make_async_copy(at(v_acc, k), at(g_txt, k), io.at[8 + k])
        return pltpu.make_async_copy(at(u_acc, 2 * k), at(g_img, k), io.at[12 + k])

    def finish_item(n, item):
        txt, k = item
        acc = v_acc if txt else u_acc
        own_row = (k if txt else 2 * k) * TILE
        far_rows = [(4 + k) * TILE] if txt else [(8 + 2 * k) * TILE, (9 + 2 * k) * TILE]
        raw = raw_i(n)

        def one(m, carry):
            sl = lambda base: pl.ds(pl.multiple_of(base + m * 32, 32), 32)
            x = raw[sl(0), :].astype(jnp.float32)
            inv = lax.rsqrt(jnp.sum(x * x, axis=-1, keepdims=True))
            x = x * inv
            total = acc[sl(own_row), :]
            for base in far_rows:
                total = total + acc[sl(base), :]
            total = total * ts
            radial = jnp.sum(x * total, axis=-1, keepdims=True)
            acc[sl(own_row), :] = (total - x * radial) * inv
            return carry
        lax.fori_loop(0, TILE // 32, one, 0)

    items = [(1, 0), (1, 1), (1, 2), (0, 0), (0, 1), (0, 2), (1, 3), (0, 3)]
    load_item(0, items[0])
    for n, item in enumerate(items):
        if n + 1 < 6:
            load_item(n + 1, items[n + 1])
        if n >= 6:
            load_item(n, item)
        for c in loads(n, item):
            c.wait()
        finish_item(n, item)
        store_item(item).start()
    for item in items:
        store_item(item).wait()
    for k in range(NQ):
        for kind in (GX, GY, GS, FX, US):
            copy_of(kind, k).wait_send()


def main_call(par, img_emb, txt_emb):
    rows, width = img_emb.shape
    any_spec = pl.BlockSpec(memory_space=pl.ANY)
    f32 = jax.ShapeDtypeStruct((rows, width), jnp.float32)
    dma = lambda k: pltpu.SemaphoreType.DMA((k,))
    outs = [
        f32, f32,
        jax.ShapeDtypeStruct((4 * rows, width), jnp.bfloat16),
        jax.ShapeDtypeStruct((2 * rows, width), jnp.bfloat16),
        f32, f32, f32, f32,
        jax.ShapeDtypeStruct((3, 8, TILE), jnp.float32),
    ]
    return pl.pallas_call(
        main_kernel,
        out_shape=outs,
        in_specs=[pl.BlockSpec(memory_space=pltpu.SMEM), any_spec, any_spec],
        out_specs=[any_spec] * 8 + [pl.BlockSpec(memory_space=pltpu.VMEM)],
        scratch_shapes=[
            pltpu.VMEM((2, 2 * TILE, width), jnp.bfloat16),
            pltpu.VMEM((2, TILE, width), jnp.bfloat16),
            pltpu.VMEM((16 * TILE, width), jnp.float32),
            pltpu.VMEM((8 * TILE, width), jnp.float32),
            pltpu.VMEM((TILE, width), jnp.float32),
            pltpu.VMEM((2 * TILE, TILE), jnp.float32),
            pltpu.VMEM((2 * TILE, TILE), jnp.bfloat16),
            pltpu.VMEM((3, 3, 8, TILE), jnp.float32),
            dma(2), dma(2), dma(16), dma(32), dma(32), dma(6),
        ],
        cost_estimate=pl.CostEstimate(flops=6 * 8 * rows * rows * width, bytes_accessed=1 << 28, transcendentals=0),
        compiler_params=pltpu.CompilerParams(
            collective_id=0, has_side_effects=True, vmem_limit_bytes=67043328),
        name="pairs",
    )(par, img_emb, txt_emb)


def solution(mesh):
    size = mesh.shape['dp']

    def local_fn(img_emb, txt_emb, log_temp, logit_bias):
        total_rows = img_emb.shape[0] * size
        temp_scale = jnp.exp(log_temp)
        par = jnp.stack([temp_scale, logit_bias])
        grad_img, grad_txt, _, _, _, _, _, _, st = main_call(par, img_emb, txt_emb)
        sums = jnp.sum(st, axis=(1, 2)) / total_rows
        return sums[0], grad_img, grad_txt, temp_scale * sums[2], sums[1]

    return jax.shard_map(
        local_fn,
        mesh=mesh,
        in_specs=(P('dp', None), P('dp', None), P(), P()),
        out_specs=(P(), P('dp', None), P('dp', None), P(), P()),
        check_vma=False,
    )
```

```python
import functools

import jax
import jax.numpy as jnp
from jax import lax
from jax.experimental import pallas as pl
from jax.experimental.pallas import tpu as pltpu
from jax.sharding import PartitionSpec as P

TILE = 512
STRIP = 128
LOG2E = 1.4426950408889634
LN2 = 0.6931471805599453
NQ = 4
NT = (((1,), (1,)), ((), ()))
NN = (((1,), (0,)), ((), ()))
TN = (((0,), (0,)), ((), ()))
SIB, XN, YN = 1, 2, 4

SEGMENTS = (
    (0, 1, 0, 4, 4),
    (0, 1, 4, 1, 4),
    (4, 1, 0, 4, 4),
    (4, 1, 4, 2, 4),
    (4, 1, 6, 1, 1),
    (5, 1, 0, 4, 4),
    (6, 1, 4, 1, 1),
    (4, 1, 7, 1, 1),
    (7, 1, 4, 1, 1),
    (5, 1, 6, 2, 2),
    (0, 1, 5, 1, 4),
    (6, 1, 5, 1, 2),
    (6, 1, 0, 4, 4),
    (6, 1, 6, 2, 2),
    (0, 1, 6, 1, 4),
    (7, 1, 6, 1, 1),
    (7, 1, 0, 4, 4),
    (7, 1, 7, 1, 1),
    (0, 1, 7, 1, 4),
    (1, 1, 0, 4, 12),
)
FORWARD_AT = (4, 10, 18, 21)


def order():
    seq = []
    for i0, istep, j0, nj, n in SEGMENTS:
        seq += [(i0 + istep * (t // nj), j0 + t % nj) for t in range(n)]
    return seq


SEQ = order()
STEPS = len(SEQ)
assert STEPS == 64 and len(set(SEQ)) == 64


def tile_of(step):
    start = 0
    vals = None
    for i0, istep, j0, nj, n in SEGMENTS:
        cur = (i0, istep, j0, nj, start)
        if vals is None:
            vals = [jnp.int32(c) for c in cur]
        else:
            vals = [jnp.where(step >= start, c, v) for c, v in zip(cur, vals)]
        start += n
    i0, istep, j0, nj, st = vals
    t = step - st
    q = jnp.where(nj == 1, t, jnp.where(nj == 2, t // 2, t // 4))
    return i0 + istep * q, j0 + (t - q * nj)


def dotf(a, b, dims):
    return lax.dot_general(a, b, dims, preferred_element_type=jnp.float32)


def at(ref, k, n=TILE):
    start = k * n
    if not isinstance(start, int):
        start = pl.multiple_of(start, n)
    return ref.at[pl.ds(start, n)]


def main_kernel(par, img_in, txt_in, g_img, g_txt, img_all, txt_all, u_sib, u_far, v_far, u_tmp, st_out,
                img_s, txt_s, u_acc, v_acc, tmp, s_buf, h_buf, st_rx,
                ld_i, ld_t, io, s_sem, r_sem, st_sem):
    me = lax.axis_index('dp')
    bit = lambda b: jnp.where((me // b) % 2 == 0, me + b, me - b)
    peer = {b: bit(b) for b in (SIB, XN, YN)}

    GX, GY, GS, FX, SU, SX, SV, US = (NQ * k for k in range(8))

    def remote(src, dst, cid, b):
        return pltpu.make_async_remote_copy(
            src_ref=src, dst_ref=dst, send_sem=s_sem.at[cid], recv_sem=r_sem.at[cid],
            device_id=(peer[b],), device_id_type=pl.DeviceIdType.MESH)

    def copy_of(kind, k):
        if kind == GX:
            return remote(at(img_all, 2 * k), at(img_all, 8 + 2 * k), GX + k, XN)
        if kind == GY:
            return remote(at(txt_all, k), at(txt_all, 4 + k), GY + k, YN)
        if kind == GS:
            return remote(at(img_all, 2 * k), at(img_all, 2 * k + 1), GS + k, SIB)
        if kind == FX:
            return remote(at(img_all, 8 + 2 * k), at(img_all, 9 + 2 * k), FX + k, SIB)
        if kind == SU:
            return remote(at(u_acc, 9 + 2 * k), at(u_tmp, k), SU + k, SIB)
        if kind == SX:
            return remote(at(u_acc, 8 + 2 * k), at(u_far, k), SX + k, XN)
        if kind == SV:
            return remote(at(v_acc, 4 + k), at(v_far, k), SV + k, YN)
        return remote(at(u_acc, 2 * k + 1), at(u_sib, k), US + k, SIB)

    raw_i = lambda t: img_s.at[t % 2, pl.ds(0, TILE)]

    def load_raw(t):
        return (pltpu.make_async_copy(at(img_in, t), raw_i(t), ld_i.at[t % 2]),
                pltpu.make_async_copy(at(txt_in, t), txt_s.at[t % 2], ld_t.at[t % 2]))

    def store_unit(t):
        return (pltpu.make_async_copy(raw_i(t), at(img_all, 2 * t), io.at[2 * (t % 2)]),
                pltpu.make_async_copy(txt_s.at[t % 2], at(txt_all, t), io.at[2 * (t % 2) + 1]))

    def fetch(i, j, slot):
        return (pltpu.make_async_copy(at(img_all, i, 2 * TILE), img_s.at[slot], ld_i.at[slot]),
                pltpu.make_async_copy(at(txt_all, j), txt_s.at[slot], ld_t.at[slot]))

    def unit_rows(buf):
        def one(k, carry):
            sl = pl.ds(pl.multiple_of(k * STRIP, STRIP), STRIP)
            x = buf[sl, :].astype(jnp.float32)
            inv = lax.rsqrt(jnp.sum(x * x, axis=-1, keepdims=True))
            buf[sl, :] = (x * inv).astype(jnp.bfloat16)
            return carry
        lax.fori_loop(0, TILE // STRIP, one, 0)

    for t in (0, 1):
        for c in load_raw(t):
            c.start()
    def clear(acc, n):
        def one(k, carry):
            acc[pl.ds(pl.multiple_of(k * 64, 64), 64)] = jnp.zeros((64, acc.shape[1]), jnp.float32)
            return carry
        lax.fori_loop(0, n * (TILE // 64), one, 0)

    barrier = pltpu.get_barrier_semaphore()
    for b in (SIB, XN, YN):
        pl.semaphore_signal(barrier, inc=1, device_id=(peer[b],), device_id_type=pl.DeviceIdType.MESH)
    clear(u_acc, 16)
    clear(v_acc, 8)
    pl.semaphore_wait(barrier, 3)

    def send_unit(t):
        for c in store_unit(t):
            c.wait()
        for kind in (GX, GY, GS):
            copy_of(kind, t).start()

    for t in range(NQ):
        for c in load_raw(t):
            c.wait()
        unit_rows(raw_i(t))
        unit_rows(txt_s.at[t % 2])
        for c in store_unit(t):
            c.start()
        if t == 0:
            send_unit(0)
        if t >= 2:
            send_unit(t - 1)
        if t == NQ - 1:
            copy_of(GS, 0).wait_recv()
            for c in fetch(SEQ[0][0], SEQ[0][1], 0):
                c.start()
        if 1 <= t + 1 < NQ and t >= 1:
            for c in load_raw(t + 1):
                c.start()
    send_unit(NQ - 1)

    ts, bias = par[0], par[1]
    scale, shift = ts * -LOG2E, bias * -LOG2E

    st_out[...] = jnp.zeros_like(st_out)

    events = {}
    add = lambda s, f: events.setdefault(s, []).append(f)
    first_i, first_j, last_i, last_j = {}, {}, {}, {}
    for s, (i, j) in enumerate(SEQ):
        first_i.setdefault(i, s)
        first_j.setdefault(j, s)
        last_i[i], last_j[j] = s, s
    wait_in = lambda kind, k: (lambda: copy_of(kind, k).wait_recv())
    start = lambda kind, k: (lambda: copy_of(kind, k).start())
    tmp_load = lambda k: pltpu.make_async_copy(at(u_tmp, k), tmp, io.at[0])

    def reduce_end(k):
        tmp_load(k).wait()

        def one(n, carry):
            sl = pl.ds(pl.multiple_of(n * 64, 64), 64)
            dst = pl.ds(pl.multiple_of((8 + 2 * k) * TILE + n * 64, 64), 64)
            u_acc[dst, :] = u_acc[dst, :] + tmp[sl, :]
            return carry
        lax.fori_loop(0, TILE // 64, one, 0)
        copy_of(SX, k).start()

    def reduce_far(k):
        copy_of(SU, k).wait_recv()
        tmp_load(k).start()
        reduce_end(k)

    for k in range(NQ):
        add(FORWARD_AT[k], wait_in(GX, k))
        add(FORWARD_AT[k], start(FX, k))
        if k:
            add(first_i[k] - 1, wait_in(GS, k))
        add(first_i[4 + k] - 1, wait_in(FX, k))
        add(first_j[4 + k] - 1, wait_in(GY, k))
        assert FORWARD_AT[k] < first_i[4 + k]
        add(last_i[4 + k] + 1, start(SU, k))
        add(last_i[4 + k] + 2, functools.partial(reduce_far, k))
        add(last_j[4 + k] + 1, start(SV, k))
        add(last_i[k] + 1, start(US, k))
    late = [f for s in sorted(events) if s >= STEPS for f in events[s]]
    events = {s: fs for s, fs in sorted(events.items()) if s < STEPS}

    def body(step, carry):
        i, j, slot = carry
        any_event = functools.reduce(jnp.logical_or, [step == s for s in events])

        @pl.when(any_event)
        def _():
            for s, fs in events.items():
                @pl.when(step == s)
                def _(fs=fs):
                    for f in fs:
                        f()

        ni, nj = tile_of(step + 1)
        nslot = 1 - slot

        @pl.when(step + 1 < STEPS)
        def _():
            for c in fetch(ni, nj, nslot):
                c.start()
        for c in fetch(i, j, slot):
            c.wait()

        a_ref, b_ref = img_s.at[slot], txt_s.at[slot]
        u_ref, v_ref = at(u_acc, i, 2 * TILE), at(v_acc, j)
        s_buf[...] = dotf(a_ref[...], b_ref[...], NT)
        soft = pos = wsum = wsim = jnp.zeros((8, TILE), jnp.float32)
        own_tile = jnp.logical_and(i == j, i < 4)
        grp = lambda x: [x[k * 8:(k + 1) * 8] for k in range(STRIP // 8)]
        for r in range(0, 2 * TILE, STRIP):
            rid = lax.broadcasted_iota(jnp.int32, (STRIP, 128), 0)
            own = jnp.logical_and(rid == lax.broadcasted_iota(jnp.int32, (STRIP, 128), 1), own_tile)

            def flip(x):
                if r >= TILE:
                    return x
                mid = x[:, r:r + 128]
                parts = [x[:, :r]] * (r > 0) + [jnp.where(own, -mid, mid)] + [x[:, r + 128:]] * (r + 128 < TILE)
                return jnp.concatenate(parts, axis=1)

            s = s_buf[r:r + STRIP]
            neg = flip(s * scale + shift)
            w = 1.0 / (1.0 + jnp.exp2(neg))
            m = jnp.minimum(w, 1.0 - w)
            h = flip(w)
            h_buf[r:r + STRIP] = h.astype(jnp.bfloat16)
            prods = grp(m)
            while len(prods) > 2:
                prods = [p + q - p * q for p, q in zip(prods[::2], prods[1::2])]
            for p in prods:
                soft = soft + jnp.log1p(-p)
            for x in grp(jnp.minimum(neg, 0.0)):
                pos = pos + x
            for x in grp(h):
                wsum = wsum + x
            for x in grp(h * s):
                wsim = wsim + x
        for n, x in enumerate((soft, pos, wsum, wsim)):
            st_out[n] += x
        h = h_buf[...]
        u_ref[...] += dotf(h, b_ref[...], NN)
        v_ref[...] += dotf(h, a_ref[...], TN)
        return ni, nj, nslot

    lax.fori_loop(0, STEPS, body, (jnp.int32(SEQ[0][0]), jnp.int32(SEQ[0][1]), jnp.int32(0)))
    for f in late:
        f()
    def share(n):
        b = (SIB, XN, YN)[n]
        return pltpu.make_async_remote_copy(
            src_ref=st_out, dst_ref=st_rx.at[n], send_sem=st_sem.at[n], recv_sem=st_sem.at[3 + n],
            device_id=(peer[b],), device_id_type=pl.DeviceIdType.MESH)

    def share_end(n):
        share(n).wait()
        st_out[...] = st_out[...] + st_rx[n]

    def loads(n, item):
        txt, k = item
        emb = pltpu.make_async_copy(at(txt_in if txt else img_in, k), raw_i(n), ld_i.at[n % 2])
        if txt:
            return emb, pltpu.make_async_copy(at(v_far, k), at(v_acc, 4 + k), io.at[4 + n % 2])
        return (emb, pltpu.make_async_copy(at(u_far, k), at(u_acc, 8 + 2 * k), io.at[4 + n % 2]),
                pltpu.make_async_copy(at(u_sib, k), at(u_acc, 9 + 2 * k), io.at[6 + n % 2]))

    def load_item(n, item):
        txt, k = item
        for kind in ((SV,) if txt else (US, SX)):
            copy_of(kind, k).wait_recv()
        for kind in ((SV,) if txt else (SU, SX)):
            copy_of(kind, k).wait_send()
        for c in loads(n, item):
            c.start()

    def store_item(item):
        txt, k = item
        if txt:
            return pltpu.make_async_copy(at(v_acc, k), at(g_txt, k), io.at[8 + k])
        return pltpu.make_async_copy(at(u_acc, 2 * k), at(g_img, k), io.at[12 + k])

    def finish_item(n, item):
        txt, k = item
        acc = v_acc if txt else u_acc
        own_row = (k if txt else 2 * k) * TILE
        far_rows = [(4 + k) * TILE] if txt else [(8 + 2 * k) * TILE, (9 + 2 * k) * TILE]
        raw = raw_i(n)

        def one(m, carry):
            sl = lambda base: pl.ds(pl.multiple_of(base + m * STRIP, STRIP), STRIP)
            x = raw[sl(0), :].astype(jnp.float32)
            inv = lax.rsqrt(jnp.sum(x * x, axis=-1, keepdims=True))
            x = x * inv
            total = acc[sl(own_row), :]
            for base in far_rows:
                total = total + acc[sl(base), :]
            total = total * ts
            radial = jnp.sum(x * total, axis=-1, keepdims=True)
            acc[sl(own_row), :] = (total - x * radial) * inv
            return carry
        lax.fori_loop(0, TILE // STRIP, one, 0)

    items = [(1, 0), (1, 1), (1, 2), (0, 0), (0, 1), (0, 2), (1, 3), (0, 3)]
    share(0).start()
    load_item(0, items[0])
    for n, item in enumerate(items):
        if n + 1 < 6:
            load_item(n + 1, items[n + 1])
        if n >= 6:
            load_item(n, item)
        for c in loads(n, item):
            c.wait()
        finish_item(n, item)
        store_item(item).start()
        if n in (1, 3, 5):
            share_end(n // 2)
            if n < 5:
                share(n // 2 + 1).start()
    for item in items:
        store_item(item).wait()
    for k in range(NQ):
        for kind in (GX, GY, GS, FX, US):
            copy_of(kind, k).wait_send()


def main_call(par, img_emb, txt_emb):
    rows, width = img_emb.shape
    any_spec = pl.BlockSpec(memory_space=pl.ANY)
    f32 = jax.ShapeDtypeStruct((rows, width), jnp.float32)
    dma = lambda k: pltpu.SemaphoreType.DMA((k,))
    outs = [
        f32, f32,
        jax.ShapeDtypeStruct((4 * rows, width), jnp.bfloat16),
        jax.ShapeDtypeStruct((2 * rows, width), jnp.bfloat16),
        f32, f32, f32, f32,
        jax.ShapeDtypeStruct((4, 8, TILE), jnp.float32),
    ]
    return pl.pallas_call(
        main_kernel,
        out_shape=outs,
        in_specs=[pl.BlockSpec(memory_space=pltpu.SMEM), any_spec, any_spec],
        out_specs=[any_spec] * 8 + [pl.BlockSpec(memory_space=pltpu.VMEM)],
        scratch_shapes=[
            pltpu.VMEM((2, 2 * TILE, width), jnp.bfloat16),
            pltpu.VMEM((2, TILE, width), jnp.bfloat16),
            pltpu.VMEM((16 * TILE, width), jnp.float32),
            pltpu.VMEM((8 * TILE, width), jnp.float32),
            pltpu.VMEM((TILE, width), jnp.float32),
            pltpu.VMEM((2 * TILE, TILE), jnp.float32),
            pltpu.VMEM((2 * TILE, TILE), jnp.bfloat16),
            pltpu.VMEM((3, 4, 8, TILE), jnp.float32),
            dma(2), dma(2), dma(16), dma(32), dma(32), dma(6),
        ],
        cost_estimate=pl.CostEstimate(flops=6 * 8 * rows * rows * width, bytes_accessed=1 << 28, transcendentals=0),
        compiler_params=pltpu.CompilerParams(
            collective_id=0, has_side_effects=True, vmem_limit_bytes=67043328),
        name="pairs",
    )(par, img_emb, txt_emb)


def solution(mesh):
    size = mesh.shape['dp']

    def local_fn(img_emb, txt_emb, log_temp, logit_bias):
        total_rows = img_emb.shape[0] * size
        temp_scale = jnp.exp(log_temp)
        par = jnp.stack([temp_scale, logit_bias])
        grad_img, grad_txt, _, _, _, _, _, _, st = main_call(par, img_emb, txt_emb)
        sums = jnp.sum(st, axis=(1, 2)) / total_rows
        loss = -(sums[0] + LN2 * sums[1])
        return loss, grad_img, grad_txt, temp_scale * sums[3], sums[2]

    return jax.shard_map(
        local_fn,
        mesh=mesh,
        in_specs=(P('dp', None), P('dp', None), P(), P()),
        out_specs=(P(), P('dp', None), P('dp', None), P(), P()),
        check_vma=False,
    )
```

```python
import functools

import jax
import jax.numpy as jnp
from jax import lax
from jax.experimental import pallas as pl
from jax.experimental.pallas import tpu as pltpu
from jax.sharding import PartitionSpec as P

TILE = 512
STRIP = 128
ROWS = 128
LOG2E = 1.4426950408889634
LN2 = 0.6931471805599453
NQ = 4
NT = (((1,), (1,)), ((), ()))
NN = (((1,), (0,)), ((), ()))
TN = (((0,), (0,)), ((), ()))
SIB, XN, YN = 1, 2, 4

SEGMENTS = (
    (0, 1, 0, 4, 4),
    (0, 1, 4, 1, 4),
    (4, 1, 0, 4, 4),
    (4, 1, 4, 2, 4),
    (4, 1, 6, 1, 1),
    (5, 1, 0, 4, 4),
    (6, 1, 4, 1, 1),
    (4, 1, 7, 1, 1),
    (7, 1, 4, 1, 1),
    (5, 1, 6, 2, 2),
    (0, 1, 5, 1, 4),
    (6, 1, 5, 1, 2),
    (6, 1, 0, 4, 4),
    (6, 1, 6, 2, 2),
    (0, 1, 6, 1, 4),
    (7, 1, 6, 1, 1),
    (7, 1, 0, 4, 4),
    (7, 1, 7, 1, 1),
    (0, 1, 7, 1, 4),
    (1, 1, 0, 4, 12),
)
FORWARD_AT = (4, 10, 18, 21)


def order():
    seq = []
    for i0, istep, j0, nj, n in SEGMENTS:
        seq += [(i0 + istep * (t // nj), j0 + t % nj) for t in range(n)]
    return seq


SEQ = order()
STEPS = len(SEQ)
assert STEPS == 64 and len(set(SEQ)) == 64


def tile_of(step):
    start = 0
    vals = None
    for i0, istep, j0, nj, n in SEGMENTS:
        cur = (i0, istep, j0, nj, start)
        if vals is None:
            vals = [jnp.int32(c) for c in cur]
        else:
            vals = [jnp.where(step >= start, c, v) for c, v in zip(cur, vals)]
        start += n
    i0, istep, j0, nj, st = vals
    t = step - st
    q = jnp.where(nj == 1, t, jnp.where(nj == 2, t // 2, t // 4))
    return i0 + istep * q, j0 + (t - q * nj)


def dotf(a, b, dims):
    return lax.dot_general(a, b, dims, preferred_element_type=jnp.float32)


def at(ref, k, n=TILE):
    start = k * n
    if not isinstance(start, int):
        start = pl.multiple_of(start, n)
    return ref.at[pl.ds(start, n)]


def main_kernel(par, img_in, txt_in, g_img, g_txt, img_all, txt_all, u_sib, u_far, v_far, u_tmp, st_out,
                img_s, txt_s, u_acc, v_acc, tmp, s_buf, h_buf, st_rx,
                ld_i, ld_t, io, s_sem, r_sem, st_sem):
    me = lax.axis_index('dp')
    bit = lambda b: jnp.where((me // b) % 2 == 0, me + b, me - b)
    peer = {b: bit(b) for b in (SIB, XN, YN)}

    GX, GY, GS, FX, SU, SX, SV, US = (NQ * k for k in range(8))

    def remote(src, dst, cid, b):
        return pltpu.make_async_remote_copy(
            src_ref=src, dst_ref=dst, send_sem=s_sem.at[cid], recv_sem=r_sem.at[cid],
            device_id=(peer[b],), device_id_type=pl.DeviceIdType.MESH)

    def copy_of(kind, k):
        if kind == GX:
            return remote(at(img_all, 2 * k), at(img_all, 8 + 2 * k), GX + k, XN)
        if kind == GY:
            return remote(at(txt_all, k), at(txt_all, 4 + k), GY + k, YN)
        if kind == GS:
            return remote(at(img_all, 2 * k), at(img_all, 2 * k + 1), GS + k, SIB)
        if kind == FX:
            return remote(at(img_all, 8 + 2 * k), at(img_all, 9 + 2 * k), FX + k, SIB)
        if kind == SU:
            return remote(at(u_acc, 9 + 2 * k), at(u_tmp, k), SU + k, SIB)
        if kind == SX:
            return remote(at(u_acc, 8 + 2 * k), at(u_far, k), SX + k, XN)
        if kind == SV:
            return remote(at(v_acc, 4 + k), at(v_far, k), SV + k, YN)
        return remote(at(u_acc, 2 * k + 1), at(u_sib, k), US + k, SIB)

    raw_i = lambda t: img_s.at[t % 2, pl.ds(0, TILE)]

    def load_raw(t):
        return (pltpu.make_async_copy(at(img_in, t), raw_i(t), ld_i.at[t % 2]),
                pltpu.make_async_copy(at(txt_in, t), txt_s.at[t % 2], ld_t.at[t % 2]))

    def store_unit(t):
        return (pltpu.make_async_copy(raw_i(t), at(img_all, 2 * t), io.at[2 * (t % 2)]),
                pltpu.make_async_copy(txt_s.at[t % 2], at(txt_all, t), io.at[2 * (t % 2) + 1]))

    def fetch(i, j, slot):
        return (pltpu.make_async_copy(at(img_all, i, 2 * TILE), img_s.at[slot], ld_i.at[slot]),
                pltpu.make_async_copy(at(txt_all, j), txt_s.at[slot], ld_t.at[slot]))

    def unit_rows(buf):
        def one(k, carry):
            sl = pl.ds(pl.multiple_of(k * STRIP, STRIP), STRIP)
            x = buf[sl, :].astype(jnp.float32)
            inv = lax.rsqrt(jnp.sum(x * x, axis=-1, keepdims=True))
            buf[sl, :] = (x * inv).astype(jnp.bfloat16)
            return carry
        lax.fori_loop(0, TILE // STRIP, one, 0)

    for t in (0, 1):
        for c in load_raw(t):
            c.start()
    def clear(acc, n):
        def one(k, carry):
            acc[pl.ds(pl.multiple_of(k * 64, 64), 64)] = jnp.zeros((64, acc.shape[1]), jnp.float32)
            return carry
        lax.fori_loop(0, n * (TILE // 64), one, 0)

    barrier = pltpu.get_barrier_semaphore()
    for b in (SIB, XN, YN):
        pl.semaphore_signal(barrier, inc=1, device_id=(peer[b],), device_id_type=pl.DeviceIdType.MESH)
    clear(u_acc, 16)
    clear(v_acc, 8)
    pl.semaphore_wait(barrier, 3)

    def send_unit(t):
        for c in store_unit(t):
            c.wait()
        for kind in (GX, GY, GS):
            copy_of(kind, t).start()

    for t in range(NQ):
        for c in load_raw(t):
            c.wait()
        unit_rows(raw_i(t))
        unit_rows(txt_s.at[t % 2])
        for c in store_unit(t):
            c.start()
        if t == 0:
            send_unit(0)
        if t >= 2:
            send_unit(t - 1)
        if t == NQ - 1:
            copy_of(GS, 0).wait_recv()
            for c in fetch(SEQ[0][0], SEQ[0][1], 0):
                c.start()
        if 1 <= t + 1 < NQ and t >= 1:
            for c in load_raw(t + 1):
                c.start()
    send_unit(NQ - 1)

    ts, bias = par[0], par[1]
    scale, shift = ts * -LOG2E, bias * -LOG2E

    st_out[...] = jnp.zeros_like(st_out)

    events = {}
    add = lambda s, f: events.setdefault(s, []).append(f)
    first_i, first_j, last_i, last_j = {}, {}, {}, {}
    for s, (i, j) in enumerate(SEQ):
        first_i.setdefault(i, s)
        first_j.setdefault(j, s)
        last_i[i], last_j[j] = s, s
    wait_in = lambda kind, k: (lambda: copy_of(kind, k).wait_recv())
    start = lambda kind, k: (lambda: copy_of(kind, k).start())
    tmp_load = lambda k: pltpu.make_async_copy(at(u_tmp, k), tmp, io.at[0])

    def reduce_end(k):
        tmp_load(k).wait()

        def one(n, carry):
            sl = pl.ds(pl.multiple_of(n * 64, 64), 64)
            dst = pl.ds(pl.multiple_of((8 + 2 * k) * TILE + n * 64, 64), 64)
            u_acc[dst, :] = u_acc[dst, :] + tmp[sl, :]
            return carry
        lax.fori_loop(0, TILE // 64, one, 0)
        copy_of(SX, k).start()

    def reduce_far(k):
        copy_of(SU, k).wait_recv()
        tmp_load(k).start()
        reduce_end(k)

    far_v = lambda k: pltpu.make_async_copy(at(v_far, k), at(v_acc, 4 + k), io.at[4 + k])
    far_u = lambda k: pltpu.make_async_copy(at(u_far, k), at(u_acc, 8 + 2 * k), io.at[8 + k])
    sib_u = lambda k: pltpu.make_async_copy(at(u_sib, k), at(u_acc, 9 + 2 * k), io.at[12 + k])

    def bring(copy, k, arrives, leaves):
        copy_of(arrives, k).wait_recv()
        copy_of(leaves, k).wait_send()
        copy(k).start()

    bring_v = lambda k: bring(far_v, k, SV, SV)
    bring_u = lambda k: bring(far_u, k, SX, SX)
    bring_sib = lambda k: bring(sib_u, k, US, SU)
    for f, k, s in ((bring_v, 0, 57), (bring_u, 0, 57), (bring_v, 1, 58), (bring_u, 1, 58), (bring_sib, 0, 59),
                    (bring_sib, 1, 60), (bring_v, 2, 62), (bring_u, 2, 62)):
        add(s, functools.partial(f, k))
    for k in range(NQ):
        add(FORWARD_AT[k], wait_in(GX, k))
        add(FORWARD_AT[k], start(FX, k))
        if k:
            add(first_i[k] - 1, wait_in(GS, k))
        add(first_i[4 + k] - 1, wait_in(FX, k))
        add(first_j[4 + k] - 1, wait_in(GY, k))
        assert FORWARD_AT[k] < first_i[4 + k]
        add(last_i[4 + k] + 1, start(SU, k))
        add(last_i[4 + k] + 2, functools.partial(reduce_far, k))
        add(last_j[4 + k] + 1, start(SV, k))
        add(last_i[k] + 1, start(US, k))
    late = [f for s in sorted(events) if s >= STEPS for f in events[s]]
    events = {s: fs for s, fs in sorted(events.items()) if s < STEPS}

    def body(step, carry):
        i, j, slot = carry
        any_event = functools.reduce(jnp.logical_or, [step == s for s in events])

        @pl.when(any_event)
        def _():
            for s, fs in events.items():
                @pl.when(step == s)
                def _(fs=fs):
                    for f in fs:
                        f()

        ni, nj = tile_of(step + 1)
        nslot = 1 - slot

        @pl.when(step + 1 < STEPS)
        def _():
            for c in fetch(ni, nj, nslot):
                c.start()
        for c in fetch(i, j, slot):
            c.wait()

        a_ref, b_ref = img_s.at[slot], txt_s.at[slot]
        u_ref, v_ref = at(u_acc, i, 2 * TILE), at(v_acc, j)
        s_buf[...] = dotf(a_ref[...], b_ref[...], NT)
        soft = pos = wsum = wsim = jnp.zeros((8, TILE), jnp.float32)
        own_tile = jnp.logical_and(i == j, i < 4)
        grp = lambda x: [x[k * 8:(k + 1) * 8] for k in range(STRIP // 8)]
        for r in range(0, 2 * TILE, STRIP):
            rid = lax.broadcasted_iota(jnp.int32, (STRIP, 128), 0)
            own = jnp.logical_and(rid == lax.broadcasted_iota(jnp.int32, (STRIP, 128), 1), own_tile)

            def flip(x):
                if r >= TILE:
                    return x
                mid = x[:, r:r + 128]
                parts = [x[:, :r]] * (r > 0) + [jnp.where(own, -mid, mid)] + [x[:, r + 128:]] * (r + 128 < TILE)
                return jnp.concatenate(parts, axis=1)

            s = s_buf[r:r + STRIP]
            neg = flip(s * scale + shift)
            w = 1.0 / (1.0 + jnp.exp2(neg))
            m = jnp.minimum(w, 1.0 - w)
            h = flip(w)
            h_buf[r:r + STRIP] = h.astype(jnp.bfloat16)
            prods = grp(m)
            while len(prods) > 2:
                prods = [p + q - p * q for p, q in zip(prods[::2], prods[1::2])]
            for p in prods:
                soft = soft + jnp.log1p(-p)
            for x in grp(jnp.minimum(neg, 0.0)):
                pos = pos + x
            for x in grp(h):
                wsum = wsum + x
            for x in grp(h * s):
                wsim = wsim + x
        for n, x in enumerate((soft, pos, wsum, wsim)):
            st_out[n] += x
        h = h_buf[...]
        u_ref[...] += dotf(h, b_ref[...], NN)
        v_ref[...] += dotf(h, a_ref[...], TN)
        return ni, nj, nslot

    lax.fori_loop(0, STEPS, body, (jnp.int32(SEQ[0][0]), jnp.int32(SEQ[0][1]), jnp.int32(0)))
    for f in late:
        f()
    def share(n):
        b = (SIB, XN, YN)[n]
        return pltpu.make_async_remote_copy(
            src_ref=st_out, dst_ref=st_rx.at[n], send_sem=st_sem.at[n], recv_sem=st_sem.at[3 + n],
            device_id=(peer[b],), device_id_type=pl.DeviceIdType.MESH)

    def share_end(n):
        share(n).wait()
        st_out[...] = st_out[...] + st_rx[n]

    def raw_of(txt, k):
        if not txt:
            return img_s.at[k // 2, pl.ds((k % 2) * TILE, TILE)]
        return txt_s.at[k % 2]

    def load_emb(txt, k):
        return pltpu.make_async_copy(at(txt_in if txt else img_in, k), raw_of(txt, k), io.at[24 + 4 * txt + k])

    def store_item(txt, k):
        if txt:
            return pltpu.make_async_copy(at(v_acc, k), at(g_txt, k), io.at[20 + k])
        return pltpu.make_async_copy(at(u_acc, 2 * k), at(g_img, k), io.at[16 + k])

    def finish_item(txt, k):
        acc = v_acc if txt else u_acc
        own_row = (k if txt else 2 * k) * TILE
        far_rows = [(4 + k) * TILE] if txt else [(8 + 2 * k) * TILE, (9 + 2 * k) * TILE]
        raw = raw_of(txt, k)

        def one(m, carry):
            sl = lambda base: pl.ds(pl.multiple_of(base + m * ROWS, ROWS), ROWS)
            x = raw[sl(0), :].astype(jnp.float32)
            inv = lax.rsqrt(jnp.sum(x * x, axis=-1, keepdims=True))
            x = x * inv
            total = acc[sl(own_row), :]
            for base in far_rows:
                total = total + acc[sl(base), :]
            total = total * ts
            radial = jnp.sum(x * total, axis=-1, keepdims=True)
            acc[sl(own_row), :] = (total - x * radial) * inv
            return carry
        lax.fori_loop(0, TILE // ROWS, one, 0)

    share(0).start()
    every = [(1, 0), (1, 1), (1, 2), (0, 0), (0, 1), (0, 2), (1, 3), (0, 3)]
    for txt, k in every:
        if not txt or k < 2:
            load_emb(txt, k).start()
    bring_sib(2)
    for n, (txt, k) in enumerate(every):
        if k == 3:
            if txt:
                bring_v(3)
            else:
                bring_sib(3)
                bring_u(3)
        load_emb(txt, k).wait()
        if txt:
            far_v(k).wait()
        else:
            far_u(k).wait()
            sib_u(k).wait()
        finish_item(txt, k)
        store_item(txt, k).start()
        if txt and k < 2:
            load_emb(txt, k + 2).start()
        if n in (1, 3, 5):
            share_end(n // 2)
            if n < 5:
                share(n // 2 + 1).start()
    for txt, k in every:
        store_item(txt, k).wait()
    for k in range(NQ):
        for kind in (GX, GY, GS, FX, US):
            copy_of(kind, k).wait_send()


def main_call(par, img_emb, txt_emb):
    rows, width = img_emb.shape
    any_spec = pl.BlockSpec(memory_space=pl.ANY)
    f32 = jax.ShapeDtypeStruct((rows, width), jnp.float32)
    dma = lambda k: pltpu.SemaphoreType.DMA((k,))
    outs = [
        f32, f32,
        jax.ShapeDtypeStruct((4 * rows, width), jnp.bfloat16),
        jax.ShapeDtypeStruct((2 * rows, width), jnp.bfloat16),
        f32, f32, f32, f32,
        jax.ShapeDtypeStruct((4, 8, TILE), jnp.float32),
    ]
    return pl.pallas_call(
        main_kernel,
        out_shape=outs,
        in_specs=[pl.BlockSpec(memory_space=pltpu.SMEM), any_spec, any_spec],
        out_specs=[any_spec] * 8 + [pl.BlockSpec(memory_space=pltpu.VMEM)],
        scratch_shapes=[
            pltpu.VMEM((2, 2 * TILE, width), jnp.bfloat16),
            pltpu.VMEM((2, TILE, width), jnp.bfloat16),
            pltpu.VMEM((16 * TILE, width), jnp.float32),
            pltpu.VMEM((8 * TILE, width), jnp.float32),
            pltpu.VMEM((TILE, width), jnp.float32),
            pltpu.VMEM((2 * TILE, TILE), jnp.float32),
            pltpu.VMEM((2 * TILE, TILE), jnp.bfloat16),
            pltpu.VMEM((3, 4, 8, TILE), jnp.float32),
            dma(2), dma(2), dma(32), dma(32), dma(32), dma(6),
        ],
        cost_estimate=pl.CostEstimate(flops=6 * 8 * rows * rows * width, bytes_accessed=1 << 28, transcendentals=0),
        compiler_params=pltpu.CompilerParams(
            collective_id=0, has_side_effects=True, vmem_limit_bytes=67043328),
        name="pairs",
    )(par, img_emb, txt_emb)


def solution(mesh):
    size = mesh.shape['dp']

    def local_fn(img_emb, txt_emb, log_temp, logit_bias):
        total_rows = img_emb.shape[0] * size
        temp_scale = jnp.exp(log_temp)
        par = jnp.stack([temp_scale, logit_bias])
        grad_img, grad_txt, _, _, _, _, _, _, st = main_call(par, img_emb, txt_emb)
        sums = jnp.sum(st, axis=(1, 2)) / total_rows
        loss = -(sums[0] + LN2 * sums[1])
        return loss, grad_img, grad_txt, temp_scale * sums[3], sums[2]

    return jax.shard_map(
        local_fn,
        mesh=mesh,
        in_specs=(P('dp', None), P('dp', None), P(), P()),
        out_specs=(P(), P('dp', None), P('dp', None), P(), P()),
        check_vma=False,
    )
```
